256 devices in a mesh: groups: 2 (over z), seq: 128 (over x, y, core).
Axes of the slice: x: 8, y: 8, z: 2, core: 2. Of those that a mesh axis runs over, the one named last changes fastest.
The devices are a block of a 8x8x16 slice.
Arguments:
- hidden_in: bfloat16 [8, 4096], P('groups', 'seq'), parts along dimension 0, may hold values from -2 to 2
- in_gain: float32 [4096], replicated, may hold values from 0.5 to 1.5
- qkv_weight: bfloat16 [4096, 9216], P(None, 'seq'), may hold values from -0.09375 to 0.09375
- q_gain: float32 [128], replicated, may hold values from 0.25 to 1.75
- k_cache: bfloat16 [8, 131072, 128], P('groups', 'seq'), parts along dimension 0, may hold values from -600 to 600
- v_cache: bfloat16 [8, 131072, 128], P('groups', 'seq'), parts along dimension 0, may hold values from -6 to 6
- lengths: int32 [8], P('groups'), parts along dimension 0, may hold values from 16384 to 32768
- out_weight: bfloat16 [4, 2048, 4096], P(None, 'seq'), may hold values from -0.25 to 0.25
- post_gain: float32 [4096], replicated, may hold values from 0.5 to 1.5
- gate_weight: bfloat16 [128, 4096, 384], P('seq'), may hold values from -0.09375 to 0.09375
- up_weight: bfloat16 [128, 4096, 384], P('seq'), may hold values from -0.09375 to 0.09375
- down_weight: bfloat16 [128, 384, 4096], P('seq'), may hold values from -0.875 to 0.875
- expert_ids: int32 [8, 8], P('groups'), parts along dimension 0, may hold values from 0 to 63, as said below
- route_weight: float32 [8, 8], P('groups'), parts along dimension 0, may hold values from 0.25 to 4
Outputs:
- mixed: float32 [8, 4096], P('groups', 'seq'), parts along dimension 0
The draws below stay inside these ranges and needn't reach their ends.
There are 2 independent parts, one for each index of `groups`. The reference program is written for one: setup_inputs(seed, part) draws one part's arguments, and reference() takes and returns one part's arrays. A program takes and returns all parts, laid end to end along the dimension named above; an argument that names none is the same for every part. Nothing has to cross between parts.
Inputs may be any that keep to these rules, and one draw needn't show every extreme that they name: `expert_ids`: each row names 8 different experts.
All inputs are finite; a program needn't handle non-finite values.
Results may differ from the reference program's by a relative error of at most 0.017.
Values may be sent and summed in bfloat16 or wider, within the bound.
A program may use at most 64 MiB of HBM per device.

```python
import math
import jax
import jax.numpy as jnp
from jax import lax

D = 4096
HEADS = 64
KVH = 4
HD = 128
TOP = 8
HALF = 384
SEQS = 4
CTX_DEV = 256
CTX = 32768
EXPERTS = 64
FF_E = 768
N_SEQ = 128


def draw_k_cache(key, part):
    first_key = jax.random.fold_in(jax.random.fold_in(key, 11), 0)
    base = jnp.clip(jax.random.normal(first_key, (SEQS, KVH * CTX, HD), jnp.float32), -6.0, 6.0) * 2.5
    return base.astype(jnp.bfloat16)


def pick_row(row_key):
    return jax.random.permutation(row_key, EXPERTS)[:TOP]


def draw_expert_ids(key, part):
    row_keys = jax.random.split(jax.random.fold_in(key, 23), SEQS)
    return jax.vmap(pick_row)(row_keys).astype(jnp.int32)


def plant(array, own_key, least, top_value):
    dims = array.shape
    place = [jax.random.randint(jax.random.fold_in(own_key, axis), (), 0, dims[axis]) for axis in range(len(dims))]
    array = array.at[tuple(place)].set(least)
    longest = dims.index(max(dims))
    place[longest] = (place[longest] + 1) % dims[longest]
    return array.at[tuple(place)].set(top_value)


def strengthened(values, key, source, target, shards_of, factor):
    owner, partner = [(jnp.arange(values.shape[axis_at]) // (values.shape[axis_at] // shards_of)).reshape([-1 if axis == axis_at else 1 for axis in range(values.ndim)]) for axis_at in (source, target)]
    chosen = jax.random.permutation(key, shards_of)[partner]
    strong = (owner == chosen) | (owner == (partner + shards_of // 2) % shards_of)
    return jnp.where(strong, factor * values, values)


def steps_of(rng, shape, shards, smallest, high):
    loudness = 1.0
    for axis_at, shards_of in shards:
        steps = jax.random.uniform(jax.random.fold_in(jax.random.fold_in(rng, 6), axis_at), (shards_of,), jnp.float32, smallest / len(shards), high / len(shards))
        loudness = loudness * jnp.repeat(jnp.exp(steps), shape[axis_at] // shards_of).reshape((-1,) + (1,) * (len(shape) - 1 - axis_at))
    return loudness


def scatter_about(key, shape, width, reach, pieces=(), kind=jnp.bfloat16):
    result = jax.random.normal(key, shape, jnp.float32) * width
    if len(pieces) > 0:
        result = steps_of(key, shape, pieces, -0.22, 0.18) * result
    return jnp.clip(result, min=-reach, max=reach).astype(kind)


def noise_with(stream_key, extent, deviation, reach, shards, heavy, kind=jnp.bfloat16):
    values = deviation * jax.random.normal(stream_key, extent, jnp.float32)
    if shards:
        values = values * steps_of(stream_key, extent, shards, -0.22, 0.18)
    return jnp.clip(strengthened(values, jax.random.fold_in(stream_key, 3), *heavy), -reach, reach).astype(kind)


def setup_inputs(seed: int = 0, part: int = 0) -> dict:
    arg_keys = jax.random.split(jax.random.key(seed), 15)
    part_splits = jax.random.split(jax.random.fold_in(arg_keys[14], part), 15)
    return {
        "hidden_in": scatter_about(part_splits[0], (SEQS, D), 0.3, 2.0, ((1, 128),)),
        "in_gain": jnp.clip(1.0 + 0.1 * jax.random.normal(arg_keys[1], (D,), jnp.float32), 0.5, 1.5),
        "qkv_weight": scatter_about(arg_keys[2], (D, (HEADS + 2 * KVH) * HD), D ** -0.5, 0.09375, ((1, 128),)),
        "q_gain": jnp.clip(1.0 + 0.15 * jax.random.normal(arg_keys[3], (HD,), jnp.float32), 0.25, 1.75),
        "k_cache": draw_k_cache(jax.random.fold_in(jax.random.fold_in(arg_keys[14], part), 71), part),
        "v_cache": scatter_about(part_splits[5], (SEQS, KVH * CTX, HD), 1.0, 6.0, ((1, 128),)),
        "lengths": plant(jax.random.randint(part_splits[6], (SEQS,), CTX // 2, CTX + 1), jax.random.fold_in(part_splits[6], 1), CTX // 2, CTX).astype(jnp.int32),
        "out_weight": noise_with(arg_keys[7], (KVH, HEADS * HD // KVH, D), (HEADS * HD) ** -0.5, 0.25, ((1, 128),), (1, 2, 128, 5.5)),
        "post_gain": jnp.clip(1.0 + 0.1 * jax.random.normal(arg_keys[8], (D,), jnp.float32), 0.5, 1.5),
        "gate_weight": scatter_about(arg_keys[9], (2 * EXPERTS, D, HALF), D ** -0.5, 0.09375, ((0, 128),)),
        "up_weight": scatter_about(arg_keys[10], (2 * EXPERTS, D, HALF), D ** -0.5, 0.09375, ((0, 128),)),
        "down_weight": noise_with(arg_keys[11], (2 * EXPERTS, HALF, D), FF_E ** -0.5, 0.875, ((0, 128),), (0, 2, 128, 5.5)),
        "expert_ids": draw_expert_ids(jax.random.fold_in(jax.random.fold_in(arg_keys[14], part), 71), part),
        "route_weight": jnp.clip(jnp.exp(jax.random.uniform(part_splits[13], (SEQS, TOP), jnp.float32, math.log(0.25), math.log(4.0))), 0.25, 4.0),
    }


EPSILON = 1e-06
ROPE_BASE = 1000000.0

def rms_scale(values, gain_vec):
    mean_square = lax.optimization_barrier(jnp.mean(values * values, axis=-1, keepdims=True))
    return values * lax.rsqrt(mean_square + EPSILON) * gain_vec

def rotate(values, positions):
    half_dim = values.shape[-1] // 2
    frequency = ROPE_BASE ** (-(2.0 * jnp.arange(half_dim, dtype=jnp.float32)) / values.shape[-1])
    angles = positions.astype(jnp.float32)[:, None] * frequency[None, :]
    cosine = jnp.cos(angles)[:, None, :]
    sine_vals = jnp.sin(angles)[:, None, :]
    lower_half = values[..., :half_dim]
    upper_half = values[..., half_dim:]
    return jnp.concatenate([lower_half * cosine - upper_half * sine_vals, upper_half * cosine + lower_half * sine_vals], axis=-1)

def project_heads(qkv_all, lengths, q_gain):
    seq_count = qkv_all.shape[0]
    query_cols = HEADS * HD
    key_cols = KVH * HD
    q_raw = qkv_all[:, :query_cols].astype(jnp.float32).reshape(seq_count, HEADS, HD)
    k_raw = qkv_all[:, query_cols:query_cols + key_cols].astype(jnp.float32).reshape(seq_count, KVH, HD)
    value_new = qkv_all[:, query_cols + key_cols:].reshape(seq_count, KVH, HD)
    queries = (rotate(rms_scale(q_raw, q_gain), lengths) * HD ** (-0.5)).astype(jnp.bfloat16)
    queries = queries.reshape(seq_count, KVH, HEADS // KVH, HD)
    key_new = rotate(rms_scale(k_raw, 1.0), lengths).astype(jnp.bfloat16)
    return (queries, key_new, value_new)

def reference(hidden_in, in_gain, qkv_weight, q_gain, k_cache, v_cache, lengths, out_weight, post_gain, gate_weight, up_weight, down_weight, expert_ids, route_weight):
    normed = rms_scale(hidden_in.astype(jnp.float32), in_gain).astype(jnp.bfloat16)
    qkv_all = jnp.dot(normed, qkv_weight, preferred_element_type=jnp.float32).astype(jnp.bfloat16)
    queries, key_new, value_new = project_heads(qkv_all, lengths, q_gain)
    own_score = jnp.einsum('sgjd,sgd->sgj', queries.astype(jnp.float32), key_new.astype(jnp.float32))
    query_wide = queries.astype(jnp.float32)
    block_rows = KVH * CTX_DEV
    keys_all = k_cache.reshape(SEQS, KVH, CTX, HD)
    vals_all = v_cache.reshape(SEQS, KVH, CTX, HD)

    def block_stats(block_id):
        first_row = (block_id * block_rows).astype(jnp.int32)
        cache_keys = lax.dynamic_slice_in_dim(keys_all, first_row, block_rows, 2)
        cache_vals = lax.dynamic_slice_in_dim(vals_all, first_row, block_rows, 2)
        positions = first_row + jnp.arange(block_rows, dtype=jnp.int32)
        live_mask = (positions[None, :] < lengths[:, None])[:, None, None, :]
        scores = jnp.einsum('sgjd,sgcd->sgjc', query_wide, cache_keys.astype(jnp.float32))
        scores = jnp.where(live_mask, scores, -1e+30)
        row_top = lax.optimization_barrier(jnp.max(scores, axis=-1))
        exp_scores = jnp.where(live_mask, jnp.exp(scores - row_top[..., None]), 0.0)
        row_total = lax.optimization_barrier(jnp.sum(exp_scores, axis=-1))
        rounded = exp_scores.astype(jnp.bfloat16).astype(jnp.float32)
        block_out = jnp.einsum('sgjc,sgcd->sgjd', rounded, cache_vals.astype(jnp.float32))
        return (row_top, row_total, block_out)
    tops, totals, outs = lax.map(block_stats, jnp.arange(N_SEQ // KVH, dtype=jnp.int32))
    best = jnp.maximum(lax.optimization_barrier(jnp.max(tops, axis=0)), own_score)
    rescale = jnp.exp(tops - best[None])
    own_weight = jnp.exp(own_score - best)
    total_all = lax.optimization_barrier(jnp.sum(rescale * totals, axis=0)) + own_weight
    summed = lax.optimization_barrier(jnp.sum(rescale[..., None] * outs, axis=0)) + own_weight[..., None] * value_new.astype(jnp.float32)[:, :, None, :]
    attn = (summed / total_all[..., None]).reshape(SEQS, HEADS * HD).astype(jnp.bfloat16)
    resid = hidden_in.astype(jnp.float32) + jnp.dot(attn, out_weight.reshape(HEADS * HD, D), preferred_element_type=jnp.float32)
    post = rms_scale(resid, post_gain).astype(jnp.bfloat16)
    route = route_weight / lax.optimization_barrier(jnp.sum(route_weight, axis=-1, keepdims=True))

    def add_slab(running, slab_set):
        gate_slab, up_slab, down_slab, slab_id = slab_set
        gate_val = jnp.dot(post, gate_slab, preferred_element_type=jnp.float32)
        up_val = jnp.dot(post, up_slab, preferred_element_type=jnp.float32)
        activated = (jax.nn.silu(gate_val) * up_val).astype(jnp.bfloat16)
        slab_out = jnp.dot(activated, down_slab, preferred_element_type=jnp.float32)
        route_coef = lax.optimization_barrier(jnp.sum(jnp.where(expert_ids == slab_id // 2, route, 0.0), axis=-1))
        return (running + route_coef[:, None] * slab_out, None)
    moe, _ = lax.scan(add_slab, jnp.zeros((SEQS, D), jnp.float32), (gate_weight, up_weight, down_weight, jnp.arange(2 * EXPERTS, dtype=jnp.int32)))
    return resid + moe
```

```python
import functools
import math

import jax
import jax.numpy as jnp
import numpy as np
from jax import lax
from jax.experimental import pallas as pl
from jax.experimental.pallas import tpu as pltpu
from jax.sharding import Mesh
from jax.sharding import PartitionSpec as P

MESH = pl.DeviceIdType.MESH
BF = jnp.bfloat16
F32 = jnp.float32

HEADS = 64
KVH = 4
HD = 128
LANES = 128
SEQ = ("seq_0", "seq_1", "seq_2")
EPSILON = 1e-06
ROPE_BASE = 1000000.0


def kernel(
    nx, ny, nc,
    hid, in_gain, qkv_w, q_gain, k_hbm, v_hbm, lengths, out_w, post_gain,
    gate_w, up_w, down_w, ids, route, freq,
    out,
    ig, qw, kc, vc, ow, pg, gu, dw,
    b1s, b1, b2, xn, qk1s, qk1, qks, q2, qf,
    aos, ast, ao, asb, xo, xs, xob, xsb,
    ys, y1, y2s, y2, y3s, y3, res, pn, ms, m1, m2s, m2,
    wsem, ssem, rsem, qssem, qrsem,
):
    nrow = ny * nc
    x = lax.axis_index("seq_0")
    y = lax.axis_index("seq_1")
    c = lax.axis_index("seq_2")
    m = y * nc + c
    group_rows = nx // KVH
    g_me = x // group_rows
    dev = x * nrow + m
    block = (x % group_rows) * nrow + m
    seqs = hid.shape[0]
    width = hid.shape[1]
    qcols = qkv_w.shape[1]
    ctx = k_hbm.shape[1]
    half = gate_w.shape[2]
    nchunk = nx * nrow * width // LANES
    per_row = nchunk // nx
    share = LANES // width
    row_heads = nrow * qcols // HD
    per_group = HEADS // KVH

    def row_id(k):
        peer = lax.rem(m + k, nrow)
        return peer, {"seq_1": peer // nc, "seq_2": lax.rem(peer, nc)}

    def col_id(k):
        peer = lax.rem(x + k, nx)
        return peer, {"seq_0": peer}

    row_order = sorted(range(1, nrow), key=lambda k: -min(k, nrow - k))
    col_order = sorted(range(1, nx), key=lambda k: -min(k, nx - k))

    loads = [
        (in_gain, ig), (qkv_w, qw), (k_hbm, kc), (v_hbm, vc), (out_w, ow), (post_gain, pg),
        (gate_w.at[0], gu.at[:, pl.ds(0, half)]), (up_w.at[0], gu.at[:, pl.ds(half, half)]),
        (down_w.at[0], dw),
    ]
    loads = [pltpu.make_async_copy(s, d, wsem.at[n]) for n, (s, d) in enumerate(loads)]

    barrier = pltpu.get_barrier_semaphore()
    for k in row_order:
        pl.semaphore_signal(barrier, inc=1, device_id=row_id(k)[1], device_id_type=MESH)
    for k in col_order:
        pl.semaphore_signal(barrier, inc=1, device_id=col_id(k)[1], device_id_type=MESH)
    for load in loads:
        load.start()

    def send_row(src_of, dst, phase):
        for k in row_order:
            peer, where = row_id(k)
            pltpu.make_async_remote_copy(
                src_ref=src_of(peer), dst_ref=dst.at[m], send_sem=ssem.at[phase],
                recv_sem=rsem.at[phase], device_id=where, device_id_type=MESH,
            ).start()

    def send_col(src_of, dst, phase):
        for k in col_order:
            peer, where = col_id(k)
            pltpu.make_async_remote_copy(
                src_ref=src_of(peer), dst_ref=dst.at[x], send_sem=ssem.at[phase],
                recv_sem=rsem.at[phase], device_id=where, device_id_type=MESH,
            ).start()

    def whole(buf, phase):
        part = buf.at[pl.ds(0, buf.shape[0] - 1)]
        return pltpu.make_async_remote_copy(
            src_ref=part, dst_ref=part, send_sem=ssem.at[phase], recv_sem=rsem.at[phase],
            device_id=col_id(1)[1], device_id_type=MESH,
        )

    phases = []

    def received(buf, phase):
        phases.append((buf, phase))
        whole(buf, phase).wait_recv()

    hv = hid[...].astype(F32)
    lane = lax.broadcasted_iota(jnp.int32, (seqs, LANES), 1)
    own = jnp.where(lane // width == lax.rem(m, share), jnp.concatenate([hv] * share, axis=1), 0.0)
    b1s[...] = own.astype(BF)
    b1[m] = own.astype(BF)

    rows = lax.broadcasted_iota(jnp.int32, (seqs, LANES), 0)
    pos = jnp.zeros((seqs, LANES), jnp.int32)
    for s in range(seqs):
        pos = jnp.where(rows == s, lengths[s], pos)
    angle = pos.astype(F32) * freq[...]
    cosv = jnp.cos(angle)
    sinv = jnp.sin(angle)
    sinv = jnp.where(lane < HD // 2, -sinv, sinv)

    pl.semaphore_wait(barrier, nrow - 1 + nx - 1)

    send_row(lambda peer: b1s, b1, 0)
    received(b1, 0)
    for k in range(per_row):
        chunk = b1[share * k].astype(F32)
        for e in range(1, share):
            chunk = chunk + b1[share * k + e].astype(F32)
        b2[x, k] = chunk.astype(BF)
    send_col(lambda peer: b2.at[x], b2, 1)
    loads[0].wait()
    loads[1].wait()
    received(b2, 1)
    squares = jnp.zeros((seqs, LANES), F32)
    for n in range(nchunk):
        v = b2[n // per_row, n % per_row].astype(F32)
        squares = squares + v * v
    scale = lax.rsqrt(jnp.sum(squares, axis=1, keepdims=True) / (nchunk * LANES) + EPSILON)
    for n in range(nchunk):
        v = b2[n // per_row, n % per_row].astype(F32)
        xn[:, n * LANES : (n + 1) * LANES] = (v * scale * ig[n : n + 1, :]).astype(BF)
    qkv = jnp.dot(xn[...], qw[...], preferred_element_type=F32)
    qkv = qkv.astype(BF).astype(F32)
    shift = lax.rem(m * qcols, LANES)
    wide = jnp.concatenate([qkv, jnp.zeros((seqs, LANES - qcols), F32)], axis=1)
    wide = pltpu.roll(wide, shift, 1)
    first = jnp.where(lane >= shift, wide, 0.0).astype(BF)
    second = jnp.where(lane < shift, wide, 0.0).astype(BF)
    qk1s[0] = first
    qk1s[1] = second
    qk1[m, 0] = first
    qk1[m, 1] = second
    send_row(lambda peer: qk1s, qk1, 2)
    received(qk1, 2)
    for h in range(row_heads):
        acc = None
        for d in range(nrow):
            at = d * qcols // LANES
            for e in range(2):
                if at + e == h and (e == 0 or (d + 1) * qcols > (at + 1) * LANES):
                    piece = qk1[d, e].astype(F32)
                    acc = piece if acc is None else acc + piece
        head = row_heads * x + h
        is_q = head < HEADS
        is_v = head >= HEADS + KVH
        mean_sq = jnp.mean(acc * acc, axis=1, keepdims=True)
        gain = jnp.where(is_q, q_gain[...], 1.0)
        normed = acc * lax.rsqrt(mean_sq + EPSILON) * gain
        turned = normed * cosv + pltpu.roll(normed, HD // 2, 1) * sinv
        turned = turned * jnp.where(is_q, HD ** -0.5, 1.0)
        qks[h] = jnp.where(is_v, acc, turned).astype(BF)

    def head_sends(act):
        for h in range(row_heads):
            head = row_heads * x + h
            extra = head >= HEADS
            group = jnp.where(extra, lax.rem(head, KVH), head // per_group)
            slot = jnp.where(extra, per_group + (head - HEADS) // KVH, lax.rem(head, per_group))
            for e in range(group_rows):
                act(h, e, group_rows * group + e, slot)

    def head_start(h, e, target, slot):
        @pl.when(target != x)
        def _():
            pltpu.make_async_remote_copy(
                src_ref=qks.at[h], dst_ref=q2.at[slot], send_sem=qssem.at[h, e],
                recv_sem=qrsem.at[slot], device_id={"seq_0": target}, device_id_type=MESH,
            ).start()

        @pl.when(target == x)
        def _():
            q2[slot] = qks[h]

    def head_sent(h, e, target, slot):
        @pl.when(target != x)
        def _():
            pltpu.make_async_remote_copy(
                src_ref=qks.at[h], dst_ref=q2.at[slot], send_sem=qssem.at[h, e],
                recv_sem=qrsem.at[slot], device_id={"seq_0": target}, device_id_type=MESH,
            ).wait_send()

    def head_wait(slot):
        if slot < per_group:
            head = g_me * per_group + slot
        else:
            head = HEADS + (slot - per_group) * KVH + g_me

        @pl.when(head // row_heads != x)
        def _():
            pltpu.make_async_remote_copy(
                src_ref=qks.at[0], dst_ref=q2.at[slot], send_sem=qssem.at[0, 0],
                recv_sem=qrsem.at[slot], device_id=col_id(1)[1], device_id_type=MESH,
            ).wait_recv()

    head_sends(head_start)
    loads[2].wait()
    loads[3].wait()
    for slot in range(per_group):
        head_wait(slot)
    for j in range(per_group):
        qf[j] = q2[j].astype(F32)
    place = block * ctx + lax.broadcasted_iota(jnp.int32, (per_group, ctx), 1)
    states = []
    for s in range(seqs):
        qs = qf[:, s, :].astype(BF)
        scores = lax.dot_general(qs, kc[s], (((1,), (1,)), ((), ())), preferred_element_type=F32)
        live = place < lengths[s]
        scores = jnp.where(live, scores, -1e30)
        top = jnp.max(scores, axis=1, keepdims=True)
        probs = jnp.where(live, jnp.exp(scores - top), 0.0)
        total = jnp.sum(probs, axis=1, keepdims=True)
        part = jnp.dot(probs.astype(BF), vc[s], preferred_element_type=F32)
        states.append((qs, top, total, part))
    head_wait(per_group)
    head_wait(per_group + 1)
    tops, totals, parts = [], [], []
    for s, (qs, top, total, part) in enumerate(states):
        kn = q2[per_group].astype(F32)[s : s + 1, :]
        vn = q2[per_group + 1].astype(F32)[s : s + 1, :]
        score = jnp.sum(qs.astype(F32) * kn, axis=1, keepdims=True)
        score = jnp.where(block == 0, score, -1e30)
        high = jnp.maximum(top, score)
        keep = jnp.exp(top - high)
        mine = jnp.where(block == 0, jnp.exp(score - high), 0.0)
        tops.append(high)
        totals.append(keep * total + mine)
        parts.append(keep * part + mine * vn)
    wide_lane = lax.broadcasted_iota(jnp.int32, (seqs * per_group, LANES), 1)
    stat = jnp.where(wide_lane == 0, jnp.concatenate(tops, axis=0), jnp.concatenate(totals, axis=0))
    stat_t = stat.T[0:2]
    stat_t = jnp.concatenate([stat_t, stat_t], axis=1)
    part_t = jnp.concatenate(parts, axis=0).T
    pieces = HD // 16
    for q in range(pieces):
        both = [part_t[16 * q : 16 * q + 8], part_t[16 * q + 8 : 16 * q + 16]]
        aos[q] = jnp.concatenate(both, axis=1).astype(BF)
    ast[...] = stat_t
    asb[m] = stat_t
    send_row(lambda peer: ast, asb, 3)
    send_row(lambda peer: aos.at[lax.rem(peer, pieces)], ao, 4)
    ao[m] = aos[lax.rem(m, pieces)]
    received(asb, 3)
    received(ao, 4)

    def merged(stats, outs):
        top = functools.reduce(jnp.maximum, [t[0:1] for t in stats])
        total, acc = 0.0, 0.0
        for t, o in zip(stats, outs):
            w = jnp.exp(t[0:1] - top)
            total = total + w * t[1:2]
            acc = acc + w * o.astype(F32)
        return top, total, acc

    top, total, acc = merged([asb[d] for d in range(nrow)], [ao[d] for d in range(nrow)])
    st = jnp.concatenate([top, total], axis=0)
    xs[...] = st
    xo[...] = acc.astype(BF)
    xsb[x] = st
    xob[x] = acc.astype(BF)
    send_col(lambda peer: xs, xsb, 5)
    send_col(lambda peer: xo, xob, 6)
    loads[4].wait()
    received(xsb, 5)
    received(xob, 6)
    lines = []
    for g in range(KVH):
        span = range(g * group_rows, (g + 1) * group_rows)
        top, total, acc = merged([xsb[d] for d in span], [xob[d] for d in span])
        acc = acc / total
        lines += [acc, pltpu.roll(acc, LANES // 2, 1)]
    lines = jnp.concatenate(lines, axis=0).astype(BF)
    head = (nrow * x + m) // pieces
    pick_row = lax.broadcasted_iota(jnp.int32, (8, LANES), 0)
    pick_lane = lax.broadcasted_iota(jnp.int32, (8, LANES), 1)
    pick = jnp.where((pick_lane == per_group * pick_row + head) & (pick_row < seqs), 1.0, 0.0)
    attn = lax.dot_general(
        pick.astype(BF), lines, (((1,), (1,)), ((), ())), preferred_element_type=F32
    ).astype(BF)
    proj = jnp.dot(attn, ow[...].reshape(-1, ow.shape[2]), preferred_element_type=F32)
    for n in range(nchunk):
        ys[n] = proj[0:seqs, n * LANES : (n + 1) * LANES]
    per_dev = nchunk // nrow
    send_row(lambda peer: ys.at[pl.ds(peer * per_dev, per_dev)], y1, 7)
    y1[m] = ys[pl.ds(m * per_dev, per_dev)]
    received(y1, 7)
    total = y1[0]
    for d in range(1, nrow):
        total = total + y1[d]
    y2s[...] = total
    y2[x] = total
    send_col(lambda peer: y2s, y2, 8)
    received(y2, 8)
    total = y2[0]
    for d in range(1, nx):
        total = total + y2[d]
    y3s[...] = total
    y3[m] = total
    send_row(lambda peer: y3s, y3, 9)
    loads[5].wait()
    loads[6].wait()
    loads[7].wait()
    received(y3, 9)
    squares = jnp.zeros((seqs, LANES), F32)
    for n in range(nchunk):
        v = b2[n // per_row, n % per_row].astype(F32) + y3[n // per_dev, n % per_dev]
        res[n] = v
        squares = squares + v * v
    scale = lax.rsqrt(jnp.sum(squares, axis=1, keepdims=True) / (nchunk * LANES) + EPSILON)
    for n in range(nchunk):
        pn[:, n * LANES : (n + 1) * LANES] = (res[n] * scale * pg[n : n + 1, :]).astype(BF)
    both = jnp.dot(pn[...], gu[...], preferred_element_type=F32)
    gate_val, up_val = both[:, :half], both[:, half:]
    act = (gate_val / (1.0 + jnp.exp(-gate_val)) * up_val).astype(BF)
    loads[8].wait()
    slab = jnp.dot(act, dw[...], preferred_element_type=F32)
    routes = route[...]
    routes = routes / jnp.sum(routes, axis=1, keepdims=True)
    coef = jnp.sum(jnp.where(ids[...] == dev // 2, routes, 0.0), axis=1, keepdims=True)
    slab = slab * coef
    for n in range(nchunk):
        ms[n] = slab[:, n * LANES : (n + 1) * LANES]
    send_col(lambda peer: ms.at[pl.ds(peer * per_row, per_row)], m1, 10)
    m1[x] = ms[pl.ds(x * per_row, per_row)]
    received(m1, 10)
    total = m1[0]
    for d in range(1, nx):
        total = total + m1[d]
    m2s[...] = total
    send_row(lambda peer: m2s.at[peer // share], m2, 11)
    m2[m] = m2s[m // share]
    received(m2, 11)
    total = res[x * per_row + m // share]
    for d in range(nrow):
        total = total + m2[d]
    at = lax.rem(m, share)
    final = total[:, 0:width]
    for e in range(1, share):
        final = jnp.where(at == e, total[:, e * width : (e + 1) * width], final)
    out[...] = final
    head_sends(head_sent)
    for buf, phase in phases:
        whole(buf, phase).wait_send()


def on_device(
    hidden_in, in_gain, qkv_weight, q_gain, k_cache, v_cache, lengths, out_weight, post_gain,
    gate_weight, up_weight, down_weight, expert_ids, route_weight,
):
    nx, ny, nc = (lax.axis_size(a) for a in SEQ)
    nrow = ny * nc
    seqs, width = hidden_in.shape
    depth = in_gain.shape[0]
    qcols = qkv_weight.shape[1]
    half = gate_weight.shape[2]
    nchunk = depth // LANES
    row_heads = nrow * qcols // HD
    per_group = HEADS // KVH
    freq = ROPE_BASE ** (-2.0 * np.arange(HD // 2) / HD)
    freq = np.concatenate([freq, freq])[None, :].astype(np.float32)
    vm = lambda *shape, t=F32: pltpu.VMEM(shape, t)
    tile = (seqs, LANES)
    per_row, per_dev = nchunk // nx, nchunk // nrow
    scratch = [
        vm(nchunk, LANES), vm(depth, qcols, t=BF), vm(*k_cache.shape, t=BF),
        vm(*v_cache.shape, t=BF), vm(*out_weight.shape, t=BF), vm(nchunk, LANES),
        vm(depth, 2 * half, t=BF), vm(half, depth, t=BF),
        vm(*tile, t=BF), vm(nrow, *tile, t=BF), vm(nx, per_row, *tile, t=BF), vm(seqs, depth, t=BF),
        vm(2, *tile, t=BF), vm(nrow, 2, *tile, t=BF), vm(row_heads, *tile, t=BF),
        vm(per_group + 2, *tile, t=BF), vm(per_group, *tile),
        vm(HD // 16, 8, LANES, t=BF), vm(2, LANES), vm(nrow, 8, LANES, t=BF), vm(nrow, 2, LANES),
        vm(8, LANES, t=BF), vm(2, LANES), vm(nx, 8, LANES, t=BF), vm(nx, 2, LANES),
        vm(nchunk, *tile), vm(nrow, per_dev, *tile), vm(per_dev, *tile), vm(nx, per_dev, *tile),
        vm(per_dev, *tile), vm(nrow, per_dev, *tile), vm(nchunk, *tile), vm(seqs, depth, t=BF),
        vm(nchunk, *tile), vm(nx, per_row, *tile), vm(per_row, *tile), vm(nrow, *tile),
        pltpu.SemaphoreType.DMA((9,)), pltpu.SemaphoreType.DMA((12,)),
        pltpu.SemaphoreType.DMA((12,)), pltpu.SemaphoreType.DMA((row_heads, nx // KVH)),
        pltpu.SemaphoreType.DMA((per_group + 2,)),
    ]
    hbm = pl.BlockSpec(memory_space=pl.ANY)
    vmem = pl.BlockSpec(memory_space=pltpu.VMEM)
    smem = pl.BlockSpec(memory_space=pltpu.SMEM)
    return pl.pallas_call(
        functools.partial(kernel, nx, ny, nc),
        out_shape=jax.ShapeDtypeStruct((seqs, width), F32),
        in_specs=[vmem, hbm, hbm, vmem, hbm, hbm, smem, hbm, hbm, hbm, hbm, hbm, vmem, vmem, vmem],
        out_specs=vmem,
        scratch_shapes=scratch,
        compiler_params=pltpu.CompilerParams(
            collective_id=0, has_side_effects=True, vmem_limit_bytes=48 * 1024 * 1024
        ),
    )(
        hidden_in, in_gain.reshape(nchunk, LANES), qkv_weight, q_gain.reshape(1, HD), k_cache,
        v_cache, lengths, out_weight, post_gain.reshape(nchunk, LANES), gate_weight, up_weight,
        down_weight, expert_ids, route_weight, jnp.asarray(freq),
    )


def solution(mesh):
    split = Mesh(
        mesh.devices.reshape(mesh.shape["groups"], 8, 8, 2), ("groups", "seq_0", "seq_1", "seq_2")
    )
    placed = (
        P("groups", SEQ),
        P(),
        P(None, SEQ),
        P(),
        P("groups", SEQ, None),
        P("groups", SEQ, None),
        P("groups"),
        P(None, SEQ, None),
        P(),
        P(SEQ, None, None),
        P(SEQ, None, None),
        P(SEQ, None, None),
        P("groups", None),
        P("groups", None),
    )
    return jax.shard_map(
        on_device, mesh=split, in_specs=placed, out_specs=P("groups", SEQ), check_vma=False
    )
```
